128 devices in a mesh: zero: 32 (over z, x, core), model: 4 (over y).
Axes of the slice: x: 4, y: 4, z: 4, core: 2. Of those that a mesh axis runs over, the one named last changes fastest.
Arguments:
- train_up: bfloat16 [12288, 49152], P('zero', 'model'), may hold values from -0.109375 to 0.109375
- low_up: bfloat16 [12288, 32], P('zero'), may hold values from -0.0546875 to 0.0546875
- high_up: bfloat16 [32, 49152], P(None, 'model'), may hold values from -1 to 1
- norm_train: float32 [12288], P(('zero', 'model')), may hold values from 0.25 to 1.75
- norm_step: float32 [12288], P(('zero', 'model')), may hold values from -0.3 to 0.3
Outputs:
- serving_up: bfloat16 [12288, 49152], P(None, ('model', 'zero'))
- scale_up: float32 [49152], P(('model', 'zero'))
- serve_norm: bfloat16 [12288], replicated
The draws below stay inside these ranges and needn't reach their ends.
All inputs are finite; a program needn't handle non-finite values. Where the reference program divides by a largest or mean magnitude, that divisor is 1e-20 or more.
Results may differ from the reference program's by a relative error of at most 0.001.
Values may be sent and summed in bfloat16 or wider, within the bound.
A program may use at most 128 MiB of HBM per device.

```python
import jax
import jax.numpy as jnp

D_MODEL = 12288
D_INNER = 49152
RANK = 32


def with_spikes(result, own_key, source, target, parts, factor):
    def block_of(dim):
        return (jnp.arange(result.shape[dim]) // (result.shape[dim] // parts)).reshape((-1,) + (1,) * (result.ndim - 1 - dim))

    near = jax.random.permutation(own_key, parts)[block_of(target)]
    far = (block_of(target) + parts // 2) % parts
    return jnp.where((block_of(source) == near) | (block_of(source) == far), factor * result, result)


def steps_of(rng, shape, shards, smallest, high):
    loudness, own = 1.0, jax.random.fold_in(rng, 6)
    for axis_at, parts in shards:
        draws = jnp.exp(jax.random.uniform(jax.random.fold_in(own, axis_at), (parts,), jnp.float32, smallest / len(shards), high / len(shards)))
        loudness = loudness * jnp.repeat(draws, shape[axis_at] // parts).reshape([-1 if axis == axis_at else 1 for axis in range(len(shape))])
    return loudness


def bell_draw(rng, dims, scale, limit, pieces=(), dtype=jnp.bfloat16):
    drawn = scale * jax.random.normal(rng, dims, jnp.float32)
    if pieces:
        drawn = drawn * steps_of(rng, dims, pieces, -0.22, 0.18)
    return jnp.clip(drawn, -limit, limit).astype(dtype)


def gaussian_with(key, shape, spread, reach, cuts, heavy, dtype=jnp.bfloat16):
    array = spread * jax.random.normal(key, shape, jnp.float32)
    if cuts:
        array = array * steps_of(key, shape, cuts, -0.22, 0.18)
    return jnp.clip(with_spikes(array, jax.random.fold_in(key, 3), *heavy), -reach, reach).astype(dtype)


def setup_inputs(seed: int = 0) -> dict:
    splits = jax.random.split(jax.random.key(seed), 6)
    train_up = gaussian_with(splits[0], (D_MODEL, D_INNER), D_MODEL ** -0.5, 0.109375, ((0, 32), (1, 4)), (0, 1, 32, 2.75))
    low_up = bell_draw(splits[1], (D_MODEL, RANK), D_MODEL ** -0.5, 0.0546875, ((0, 32),))
    high_up = bell_draw(splits[2], (RANK, D_INNER), RANK ** -0.5, 1.0, ((1, 4),))
    norm_train = jnp.clip(1.0 + 0.15 * jax.random.normal(splits[3], (D_MODEL,), jnp.float32), 0.25, 1.75)
    norm_step = jnp.clip(jax.random.uniform(splits[4], (D_MODEL,), jnp.float32, -0.3, 0.3) * steps_of(splits[4], (D_MODEL,), ((0, 128),), -0.4, 0.0), -0.3, 0.3)
    return {"train_up": train_up, "low_up": low_up, "high_up": high_up, "norm_train": norm_train, "norm_step": norm_step}


mix_rate = 0.5


def reference(train_up, low_up, high_up, norm_train, norm_step):
    whole_up = train_up.astype(jnp.float32) + mix_rate * jnp.dot(low_up, high_up, preferred_element_type=jnp.float32)
    scale_up = jnp.sum(jnp.abs(whole_up), axis=0) / D_MODEL
    serving_up = (whole_up / scale_up).astype(jnp.bfloat16)
    serve_norm = (norm_train + norm_step).astype(jnp.bfloat16)
    return serving_up, scale_up, serve_norm
```

```python
import jax
import jax.numpy as jnp
from jax import lax
from jax.experimental import pallas as pl
from jax.experimental.pallas import tpu as pltpu
from jax.sharding import Mesh
from jax.sharding import PartitionSpec as P

D_MODEL = 12288
ROWS = 384
COLS = 384
RANK = 32
PIECE = 96
ZERO = ("zero_0", "zero_1", "zero_2")
ZERO_MODEL = ("zero_0", "zero_1", "zero_2", "model")
MODEL_ZERO = ("model", "zero_0", "zero_1", "zero_2")
MESH = pl.DeviceIdType.MESH

mix_rate = 0.5

PHASES = (
    ((2, 2),),
    ((2, 0), (0, 2)),
    ((1, 1), (3, 3)),
    ((1, 3), (3, 1)),
    ((1, 2), (3, 0)),
    ((3, 2), (1, 0)),
    ((2, 1), (0, 3)),
    ((2, 3), (0, 1)),
)
BIG = ((0, 0, 1),) + tuple((z, x, c) for phase in PHASES for x, z in phase for c in range(2))
AHEAD = 3
CHIPS = tuple((z, x) for z in range(4) for x in range(4) if (z, x) != (0, 0))
TILE = 128
PART = 768


def exchange(
    train, low, high, norm_train, norm_step, whole, scale, norm,
    recv, high_mine, norm_mine, low_cols, low_all, norm_all, sums, norm_rows,
    big_send, big_recv, low_send, low_recv, norm_send, norm_recv, local_sem,
):
    z, x, core, y = (lax.axis_index(a) for a in ZERO_MODEL)
    chip = z * 4 + x
    me = chip * 2 + core

    def at(dz, dx, dc, dy=0):
        return (lax.rem(z + dz, 4), lax.rem(x + dx, 4), lax.rem(core + dc, 2), lax.rem(y + dy, 4))

    barrier = pltpu.get_barrier_semaphore()
    for dz, dx, dc in BIG:
        pl.semaphore_signal(barrier, inc=1, device_id=at(dz, dx, dc), device_id_type=MESH)
    for dy in (1, 2, 3):
        pl.semaphore_signal(barrier, inc=1, device_id=at(0, 0, 0, dy), device_id_type=MESH)

    own = pltpu.make_async_copy(
        train.at[:, pl.ds(pl.multiple_of(me * COLS, 128), COLS)],
        recv.at[pl.ds(pl.multiple_of(me * ROWS, ROWS), ROWS)],
        local_sem.at[0],
    )
    own.start()
    get_high = pltpu.make_async_copy(
        high.at[:, pl.ds(pl.multiple_of(me * COLS, 128), COLS)], high_mine, local_sem.at[1]
    )
    get_high.start()

    get_low = pltpu.make_async_copy(
        low.at[pl.ds(pl.multiple_of(y * 8, 8), 8)], low_all.at[core, y, chip], local_sem.at[2]
    )
    get_low.start()
    get_norm = [
        pltpu.make_async_copy(ref, norm_mine.at[i], local_sem.at[3 + i])
        for i, ref in enumerate((norm_train, norm_step))
    ]
    for copy in get_norm:
        copy.start()
    norm_all[core, y, chip] = jnp.zeros((1, 128), jnp.float32)
    sums[...] = jnp.zeros_like(sums)
    for copy in get_norm:
        copy.wait()
    norm_all[core, y, chip, :, pl.ds(0, PIECE)] = norm_mine[0] + norm_mine[1]

    pl.semaphore_wait(barrier, len(BIG) + 3)
    get_low.wait()

    def big(k):
        dz, dx, dc = BIG[k]
        there = at(dz, dx, dc)
        column = (there[0] * 8 + there[1] * 2 + there[2]) * COLS
        return pltpu.make_async_remote_copy(
            src_ref=train.at[:, pl.ds(pl.multiple_of(column, 128), COLS)],
            dst_ref=recv.at[pl.ds(pl.multiple_of(me * ROWS, ROWS), ROWS)],
            send_sem=big_send.at[k],
            recv_sem=big_recv.at[k],
            device_id=there,
            device_id_type=MESH,
        )

    def small(ref, send, got, k, there):
        return pltpu.make_async_remote_copy(
            src_ref=ref, dst_ref=ref, send_sem=send.at[k], recv_sem=got.at[k],
            device_id=there, device_id_type=MESH,
        )

    bigs = [big(k) for k in range(len(BIG))]
    for copy in bigs[:AHEAD]:
        copy.start()
    smalls = []
    for k, (dz, dx) in enumerate(CHIPS):
        there = at(dz, dx, 0)
        smalls.append(small(low_all.at[core, y, chip], low_send, low_recv, k, there))
        smalls.append(small(norm_all.at[core, y, chip], norm_send, norm_recv, k, there))
    for copy in smalls:
        copy.start()
    for copy in bigs[AHEAD:]:
        copy.start()

    for copy in smalls:
        copy.wait()
    smalls = []
    for dy in (1, 2, 3):
        there = at(0, 0, 0, dy)
        smalls.append(small(low_all.at[core, y], low_send, low_recv, 14 + dy, there))
        smalls.append(small(norm_all.at[core, y], norm_send, norm_recv, 14 + dy, there))
    for copy in smalls:
        copy.start()
    for copy in smalls:
        copy.wait()
    there = at(0, 0, 1)
    smalls = [
        small(low_all.at[core], low_send, low_recv, 18, there),
        small(norm_all.at[core], norm_send, norm_recv, 18, there),
    ]
    for copy in smalls:
        copy.start()
    for copy in smalls:
        copy.wait()

    for c in range(2):
        line = jnp.zeros((16, 384), jnp.float32)
        for q in range(4):
            part = norm_all[c, q].reshape(16, 128)
            part = jnp.concatenate([part, jnp.zeros((16, 256), jnp.float32)], axis=1)
            line = line + (pltpu.roll(part, q * PIECE, 1) if q else part)
        for j in range(3):
            norm_rows[pl.ds(3 * c + j, 16, stride=6), :] = line[:, j * 128 : j * 128 + 128]
    norm[...] = norm_rows[...].astype(jnp.bfloat16)

    own.wait()
    get_high.wait()
    right = (high_mine[...].astype(jnp.float32) * mix_rate).astype(jnp.bfloat16)

    def add(source_chip, source_core):
        low_cols[...] = jnp.concatenate(
            [low_all[source_core, q, source_chip].astype(jnp.float32) for q in range(4)], axis=0
        ).T.astype(jnp.bfloat16)
        first = (source_chip * 2 + source_core) * ROWS

        @pl.loop(0, ROWS // TILE)
        def _(i):
            start = pl.multiple_of(i * TILE, TILE)
            rows = pl.ds(pl.multiple_of(first + start, TILE), TILE)
            product = jnp.dot(
                low_cols[pl.ds(start, TILE)], right, preferred_element_type=jnp.float32
            )
            value = recv[rows].astype(jnp.float32) + product
            whole[rows] = value
            sums[...] += jnp.sum(jnp.abs(value).reshape(TILE // 8, 8, COLS), axis=0)

    add(chip, core)
    for k, (dz, dx, dc) in enumerate(BIG):
        bigs[k].wait_recv()
        from_z, from_x, from_core, _ = at(4 - dz, 4 - dx, dc)
        add(from_z * 4 + from_x, from_core)
    scale[...] = jnp.sum(sums[...], axis=0, keepdims=True) / D_MODEL
    for copy in bigs:
        copy.wait_send()


def finish(whole, scale, norm, serving, scale_out, norm_out, staged, sems):
    scale_out[...] = scale[0]
    norm_out[...] = norm[...]
    inverse = 1.0 / scale[...]
    copies = []
    for i in range(D_MODEL // PART):
        rows = pl.ds(i * PART, PART)

        @pl.loop(0, PART // 64)
        def _(j):
            inner = pl.ds(pl.multiple_of(i * PART + j * 64, 64), 64)
            staged[inner] = (whole[inner] * inverse).astype(jnp.bfloat16)

        copy = pltpu.make_async_copy(staged.at[rows], serving.at[rows], sems.at[i])
        copy.start()
        copies.append(copy)
    for copy in copies:
        copy.wait()


def local(train_up, low_up, high_up, norm_train, norm_step):
    vmem = pl.BlockSpec(memory_space=pltpu.VMEM)
    hbm = pl.BlockSpec(memory_space=pltpu.HBM)
    n = len(BIG)
    dma = pltpu.SemaphoreType.DMA
    inputs = (
        train_up, low_up.T, high_up, norm_train.reshape(1, PIECE), norm_step.reshape(1, PIECE)
    )
    whole, scale, norm = pl.pallas_call(
        exchange,
        name="exchange",
        out_shape=(
            pltpu.VMEM((D_MODEL, COLS), jnp.float32),
            jax.ShapeDtypeStruct((1, COLS), jnp.float32),
            jax.ShapeDtypeStruct((PIECE, 128), jnp.bfloat16),
        ),
        in_specs=[hbm] * 5,
        out_specs=(vmem, vmem, vmem),
        scratch_shapes=[
            pltpu.VMEM((D_MODEL, COLS), jnp.bfloat16),
            pltpu.VMEM((RANK, COLS), jnp.bfloat16),
            pltpu.VMEM((2, 1, PIECE), jnp.float32),
            pltpu.VMEM((ROWS, RANK), jnp.bfloat16),
            pltpu.VMEM((2, 4, 16, 8, ROWS), jnp.bfloat16),
            pltpu.VMEM((2, 4, 16, 1, 128), jnp.float32),
            pltpu.VMEM((8, COLS), jnp.float32),
            pltpu.VMEM((PIECE, 128), jnp.float32),
            dma((n,)), dma((n,)), dma((19,)), dma((19,)), dma((19,)), dma((19,)), dma((5,)),
        ],
        compiler_params=pltpu.CompilerParams(
            collective_id=0, has_side_effects=True, vmem_limit_bytes=16 << 20
        ),
        cost_estimate=pl.CostEstimate(flops=300_000_000, bytes_accessed=40_000_000, transcendentals=0),
    )(*[pltpu.with_memory_space_constraint(array, pltpu.HBM) for array in inputs])
    serving_up, scale_up, serve_norm = pl.pallas_call(
        finish,
        name="finish",
        out_shape=(
            jax.ShapeDtypeStruct((D_MODEL, COLS), jnp.bfloat16),
            jax.ShapeDtypeStruct((COLS,), jnp.float32),
            jax.ShapeDtypeStruct((PIECE, 128), jnp.bfloat16),
        ),
        in_specs=[vmem, vmem, vmem],
        out_specs=(hbm, vmem, vmem),
        scratch_shapes=[pltpu.VMEM((D_MODEL, COLS), jnp.bfloat16), dma((D_MODEL // PART,))],
        compiler_params=pltpu.CompilerParams(vmem_limit_bytes=12 << 20),
        cost_estimate=pl.CostEstimate(flops=10_000_000, bytes_accessed=10_000_000, transcendentals=0),
    )(pltpu.with_memory_space_constraint(whole, pltpu.VMEM), scale, norm)
    return serving_up, scale_up, serve_norm.reshape(D_MODEL)


def solution(mesh):
    split = Mesh(
        mesh.devices.reshape(4, 4, 2, mesh.shape["model"]), ("zero_0", "zero_1", "zero_2", "model")
    )
    placed = (P(ZERO, "model"), P(ZERO, None), P(None, "model"), P(ZERO_MODEL), P(ZERO_MODEL))
    return jax.shard_map(
        local,
        mesh=split,
        in_specs=placed,
        out_specs=(P(None, MODEL_ZERO), P(MODEL_ZERO), P()),
        check_vma=False,
    )
```

```python
import jax
import jax.numpy as jnp
from jax import lax
from jax.experimental import pallas as pl
from jax.experimental.pallas import tpu as pltpu
from jax.sharding import Mesh
from jax.sharding import PartitionSpec as P

D_MODEL = 12288
ROWS = 384
COLS = 384
RANK = 32
PIECE = 96
ZERO = ("zero_0", "zero_1", "zero_2")
ZERO_MODEL = ("zero_0", "zero_1", "zero_2", "model")
MODEL_ZERO = ("model", "zero_0", "zero_1", "zero_2")
MESH = pl.DeviceIdType.MESH

mix_rate = 0.5

PHASES = (
    ((1, 1), (3, 3)),
    ((1, 3), (3, 1)),
    ((1, 2), (3, 0)),
    ((3, 2), (1, 0)),
    ((2, 1), (0, 3)),
    ((2, 3), (0, 1)),
    ((2, 2),),
    ((2, 0), (0, 2)),
)
FIRST = 1
CHIPS = tuple((z, x) for phase in PHASES for x, z in phase)
EARLY = sum(len(phase) for phase in PHASES[:FIRST])
NEAR = ((0, 0, 1),) + tuple(
    (z, x, c) for z in (0, 1, 3) for x in (0, 1, 3) for c in range(2) if (z, x) != (0, 0)
)
TILE = 128
PARTS = (256, 512, 768) + (1536,) * 7
BODY = 256


def exchange(
    train, low, high, norm_train, norm_step, whole, scale, norm,
    recv, high_mine, norm_mine, low_cols, low_all, norm_all, sums, norm_rows,
    heard, big_send, big_recv, low_send, low_recv, norm_send, norm_recv, local_sem,
):
    z, x, core, y = (lax.axis_index(a) for a in ZERO_MODEL)
    chip = z * 4 + x
    me = chip * 2 + core

    def at(dz, dx, dc, dy=0):
        return (lax.rem(z + dz, 4), lax.rem(x + dx, 4), lax.rem(core + dc, 2), lax.rem(y + dy, 4))

    barrier = pltpu.get_barrier_semaphore()
    for dz, dx, dc in NEAR:
        pl.semaphore_signal(barrier, inc=1, device_id=at(dz, dx, dc), device_id_type=MESH)
    for dy in (1, 2, 3):
        pl.semaphore_signal(barrier, inc=1, device_id=at(0, 0, 0, dy), device_id_type=MESH)

    own = pltpu.make_async_copy(
        train.at[:, pl.ds(pl.multiple_of(me * COLS, 128), COLS)],
        recv.at[pl.ds(pl.multiple_of(me * ROWS, ROWS), ROWS)],
        local_sem.at[0],
    )
    own.start()
    get_high = pltpu.make_async_copy(
        high.at[:, pl.ds(pl.multiple_of(me * COLS, 128), COLS)], high_mine, local_sem.at[1]
    )
    get_high.start()

    get_low = pltpu.make_async_copy(
        low.at[pl.ds(pl.multiple_of(y * 8, 8), 8)], low_all.at[core, y, chip], local_sem.at[2]
    )
    get_low.start()
    get_norm = [
        pltpu.make_async_copy(ref, norm_mine.at[i], local_sem.at[3 + i])
        for i, ref in enumerate((norm_train, norm_step))
    ]
    for copy in get_norm:
        copy.start()
    norm_all[core, y, chip] = jnp.zeros((1, 128), jnp.float32)
    sums[...] = jnp.zeros_like(sums)
    for copy in get_norm:
        copy.wait()
    norm_all[core, y, chip, :, pl.ds(0, PIECE)] = norm_mine[0] + norm_mine[1]

    def big(place, i, target):
        column = (place[0] * 8 + place[1] * 2 + target) * COLS
        return pltpu.make_async_remote_copy(
            src_ref=train.at[:, pl.ds(pl.multiple_of(column, 128), COLS)],
            dst_ref=recv.at[pl.ds(pl.multiple_of(me * ROWS, ROWS), ROWS)],
            send_sem=big_send.at[2 * i + target],
            recv_sem=big_recv.at[2 * i + core],
            device_id=(place[0], place[1], target, y),
            device_id_type=MESH,
        )

    def small(ref, send, got, k, there):
        return pltpu.make_async_remote_copy(
            src_ref=ref, dst_ref=ref, send_sem=send.at[k], recv_sem=got.at[k],
            device_id=there, device_id_type=MESH,
        )

    pl.semaphore_wait(barrier, len(NEAR) + 3)
    other = pltpu.make_async_remote_copy(
        src_ref=train.at[:, pl.ds(pl.multiple_of((chip * 2 + 1 - core) * COLS, 128), COLS)],
        dst_ref=recv.at[pl.ds(pl.multiple_of(me * ROWS, ROWS), ROWS)],
        send_sem=big_send.at[30],
        recv_sem=big_recv.at[30],
        device_id=at(0, 0, 1),
        device_id_type=MESH,
    )
    bigs = [
        big(at(dz, dx, 0), i, target) for i, (dz, dx) in enumerate(CHIPS) for target in range(2)
    ]
    other.start()
    for copy in bigs[: 2 * EARLY]:
        copy.start()
    for dz, dx, dc in NEAR:
        pl.semaphore_signal(heard, inc=1, device_id=at(dz, dx, dc), device_id_type=MESH)
    get_low.wait()
    pl.semaphore_wait(heard, len(NEAR))
    smalls = []
    for k, (dz, dx) in enumerate(CHIPS):
        there = at(dz, dx, 0)
        smalls.append(small(low_all.at[core, y, chip], low_send, low_recv, k, there))
        smalls.append(small(norm_all.at[core, y, chip], norm_send, norm_recv, k, there))
    for copy in smalls:
        copy.start()
    for copy in bigs[2 * EARLY :]:
        copy.start()

    for copy in smalls:
        copy.wait()
    smalls = []
    for dy in (1, 2, 3):
        there = at(0, 0, 0, dy)
        smalls.append(small(low_all.at[core, y], low_send, low_recv, 14 + dy, there))
        smalls.append(small(norm_all.at[core, y], norm_send, norm_recv, 14 + dy, there))
    for copy in smalls:
        copy.start()
    for copy in smalls:
        copy.wait()
    there = at(0, 0, 1)
    smalls = [
        small(low_all.at[core], low_send, low_recv, 18, there),
        small(norm_all.at[core], norm_send, norm_recv, 18, there),
    ]
    for copy in smalls:
        copy.start()
    for copy in smalls:
        copy.wait()

    for c in range(2):
        line = jnp.zeros((16, 384), jnp.float32)
        for q in range(4):
            part = norm_all[c, q].reshape(16, 128)
            part = jnp.concatenate([part, jnp.zeros((16, 256), jnp.float32)], axis=1)
            line = line + (pltpu.roll(part, q * PIECE, 1) if q else part)
        for j in range(3):
            norm_rows[pl.ds(3 * c + j, 16, stride=6), :] = line[:, j * 128 : j * 128 + 128]
    norm[...] = norm_rows[...].astype(jnp.bfloat16)

    get_high.wait()
    right = (high_mine[...].astype(jnp.float32) * mix_rate).astype(jnp.bfloat16)

    @pl.loop(0, 32)
    def _(source):
        low_cols[...] = jnp.concatenate(
            [low_all[source % 2, q, source // 2].astype(jnp.float32) for q in range(4)], axis=0
        ).T.astype(jnp.bfloat16)

        @pl.loop(0, ROWS // TILE)
        def _(i):
            start = pl.multiple_of(i * TILE, TILE)
            whole[pl.ds(pl.multiple_of(source * ROWS + start, TILE), TILE)] = jnp.dot(
                low_cols[pl.ds(start, TILE)], right, preferred_element_type=jnp.float32
            )

    def add(source):
        @pl.loop(0, ROWS // TILE)
        def _(i):
            rows = pl.ds(pl.multiple_of(source * ROWS + i * TILE, TILE), TILE)
            value = recv[rows].astype(jnp.float32) + whole[rows]
            whole[rows] = value
            sums[...] += jnp.sum(jnp.abs(value).reshape(TILE // 8, 8, COLS), axis=0)

    own.wait()
    add(me)
    other.wait()
    add(chip * 2 + 1 - core)
    for i, (dz, dx) in enumerate(CHIPS):
        from_z, from_x, _, _ = at(4 - dz, 4 - dx, 0)
        for source_core in range(2):
            source = (from_z * 4 + from_x) * 2 + source_core
            pltpu.make_async_remote_copy(
                src_ref=train.at[:, pl.ds(0, COLS)],
                dst_ref=recv.at[pl.ds(pl.multiple_of(source * ROWS, ROWS), ROWS)],
                send_sem=big_send.at[2 * i + source_core],
                recv_sem=big_recv.at[2 * i + source_core],
                device_id=(from_z, from_x, source_core, y),
                device_id_type=MESH,
            ).wait_recv()
            add(source)
    scale[...] = jnp.sum(sums[...], axis=0, keepdims=True) / D_MODEL
    for copy in bigs:
        copy.wait_send()


def finish(whole, scale, norm, serving, scale_out, norm_out, staged, scale_line, sems, small_sems):
    scale_line[...] = scale[0]
    inverse = 1.0 / scale[...]
    copies = [
        pltpu.make_async_copy(scale_line, scale_out, small_sems.at[0]),
        pltpu.make_async_copy(norm, norm_out, small_sems.at[1]),
    ]
    for copy in copies:
        copy.start()
    first = 0
    for i, length in enumerate(PARTS):

        @pl.loop(0, length // BODY)
        def _(j):
            inner = pl.ds(pl.multiple_of(first + j * BODY, BODY), BODY)
            staged[inner] = (whole[inner] * inverse).astype(jnp.bfloat16)

        rows = pl.ds(first, length)
        copy = pltpu.make_async_copy(staged.at[rows], serving.at[rows], sems.at[i])
        copy.start()
        copies.append(copy)
        first += length
    for copy in copies:
        copy.wait()


def local(train_up, low_up, high_up, norm_train, norm_step):
    vmem = pl.BlockSpec(memory_space=pltpu.VMEM)
    hbm = pl.BlockSpec(memory_space=pltpu.HBM)
    dma = pltpu.SemaphoreType.DMA
    inputs = (
        train_up, low_up.T, high_up, norm_train.reshape(1, PIECE), norm_step.reshape(1, PIECE)
    )
    whole, scale, norm = pl.pallas_call(
        exchange,
        name="exchange",
        out_shape=(
            pltpu.VMEM((D_MODEL, COLS), jnp.float32),
            jax.ShapeDtypeStruct((1, COLS), jnp.float32),
            jax.ShapeDtypeStruct((PIECE, 128), jnp.bfloat16),
        ),
        in_specs=[hbm] * 5,
        out_specs=(vmem, vmem, vmem),
        scratch_shapes=[
            pltpu.VMEM((D_MODEL, COLS), jnp.bfloat16),
            pltpu.VMEM((RANK, COLS), jnp.bfloat16),
            pltpu.VMEM((2, 1, PIECE), jnp.float32),
            pltpu.VMEM((ROWS, RANK), jnp.bfloat16),
            pltpu.VMEM((2, 4, 16, 8, ROWS), jnp.bfloat16),
            pltpu.VMEM((2, 4, 16, 1, 128), jnp.float32),
            pltpu.VMEM((8, COLS), jnp.float32),
            pltpu.VMEM((PIECE, 128), jnp.float32),
            pltpu.SemaphoreType.REGULAR, dma((31,)), dma((31,)), dma((19,)), dma((19,)), dma((19,)), dma((19,)), dma((5,)),
        ],
        compiler_params=pltpu.CompilerParams(
            collective_id=0, has_side_effects=True, vmem_limit_bytes=16 << 20
        ),
        cost_estimate=pl.CostEstimate(flops=300_000_000, bytes_accessed=40_000_000, transcendentals=0),
    )(*[pltpu.with_memory_space_constraint(array, pltpu.HBM) for array in inputs])
    serving_up, scale_up, serve_norm = pl.pallas_call(
        finish,
        name="finish",
        out_shape=(
            jax.ShapeDtypeStruct((D_MODEL, COLS), jnp.bfloat16),
            jax.ShapeDtypeStruct((COLS,), jnp.float32),
            jax.ShapeDtypeStruct((PIECE, 128), jnp.bfloat16),
        ),
        in_specs=[vmem, vmem, vmem],
        out_specs=(hbm, hbm, hbm),
        scratch_shapes=[
            pltpu.VMEM((D_MODEL, COLS), jnp.bfloat16),
            pltpu.VMEM((COLS,), jnp.float32),
            dma((len(PARTS),)), dma((2,)),
        ],
        compiler_params=pltpu.CompilerParams(vmem_limit_bytes=12 << 20),
        cost_estimate=pl.CostEstimate(flops=10_000_000, bytes_accessed=10_000_000, transcendentals=0),
    )(pltpu.with_memory_space_constraint(whole, pltpu.VMEM), scale, norm)
    return serving_up, scale_up, serve_norm.reshape(D_MODEL)


def solution(mesh):
    split = Mesh(
        mesh.devices.reshape(4, 4, 2, mesh.shape["model"]), ("zero_0", "zero_1", "zero_2", "model")
    )
    placed = (P(ZERO, "model"), P(ZERO, None), P(None, "model"), P(ZERO_MODEL), P(ZERO_MODEL))
    return jax.shard_map(
        local,
        mesh=split,
        in_specs=placed,
        out_specs=(P(None, MODEL_ZERO), P(MODEL_ZERO), P()),
        check_vma=False,
    )
```

```python
import jax
import jax.numpy as jnp
from jax import lax
from jax.experimental import pallas as pl
from jax.experimental.pallas import tpu as pltpu
from jax.sharding import Mesh
from jax.sharding import PartitionSpec as P

D_MODEL = 12288
ROWS = 384
COLS = 384
RANK = 32
PIECE = 96
ZERO = ("zero_0", "zero_1", "zero_2")
ZERO_MODEL = ("zero_0", "zero_1", "zero_2", "model")
MODEL_ZERO = ("model", "zero_0", "zero_1", "zero_2")
MESH = pl.DeviceIdType.MESH

mix_rate = 0.5

PHASES = (
    ((1, 3), (3, 1)),
    ((1, 1), (3, 3)),
    ((3, 2), (1, 0)),
    ((1, 2), (3, 0)),
    ((2, 3), (0, 1)),
    ((2, 1), (0, 3)),
    ((2, 2),),
    ((2, 0), (0, 2)),
)
FIRST = 1
MORE = 4
CHIPS = tuple((z, x) for phase in PHASES for x, z in phase)
EARLY = sum(len(phase) for phase in PHASES[:FIRST])
NEAR = ((0, 0, 1),) + tuple(
    (z, x, c) for z in (0, 1, 3) for x in (0, 1, 3) for c in range(2) if (z, x) != (0, 0)
)
TILE = 128
PARTS = (256, 512, 768) + (1536,) * 7
BODY = 256


def exchange(
    train, low, high, norm_train, norm_step, whole, scale, norm,
    recv, high_mine, norm_mine, low_cols, low_all, norm_all, sums, norm_rows,
    heard, big_send, big_recv, low_send, low_recv, norm_send, norm_recv, local_sem,
):
    z, x, core, y = (lax.axis_index(a) for a in ZERO_MODEL)
    chip = z * 4 + x
    me = chip * 2 + core
    slot = chip * (1 - core) + (x * 4 + z) * core
    line = pl.ds((z * (1 - core) + x * core) * 4, 4)

    def at(dz, dx, dc, dy=0):
        return (lax.rem(z + dz, 4), lax.rem(x + dx, 4), lax.rem(core + dc, 2), lax.rem(y + dy, 4))

    barrier = pltpu.get_barrier_semaphore()
    for dz, dx, dc in NEAR:
        pl.semaphore_signal(barrier, inc=1, device_id=at(dz, dx, dc), device_id_type=MESH)
    for dy in (1, 2, 3):
        pl.semaphore_signal(barrier, inc=1, device_id=at(0, 0, 0, dy), device_id_type=MESH)

    own = pltpu.make_async_copy(
        train.at[:, pl.ds(pl.multiple_of(me * COLS, 128), COLS)],
        recv.at[pl.ds(pl.multiple_of(me * ROWS, ROWS), ROWS)],
        local_sem.at[0],
    )
    own.start()
    get_high = pltpu.make_async_copy(
        high.at[:, pl.ds(pl.multiple_of(me * COLS, 128), COLS)], high_mine, local_sem.at[1]
    )
    get_high.start()

    get_low = pltpu.make_async_copy(
        low.at[pl.ds(pl.multiple_of(y * 8, 8), 8)], low_all.at[core, y, slot], local_sem.at[2]
    )
    get_low.start()
    get_norm = [
        pltpu.make_async_copy(ref, norm_mine.at[i], local_sem.at[3 + i])
        for i, ref in enumerate((norm_train, norm_step))
    ]
    for copy in get_norm:
        copy.start()
    norm_all[core, y, slot] = jnp.zeros((1, 128), jnp.float32)
    sums[...] = jnp.zeros_like(sums)
    for copy in get_norm:
        copy.wait()
    norm_all[core, y, slot, :, pl.ds(0, PIECE)] = norm_mine[0] + norm_mine[1]

    def big(place, i, target):
        column = (place[0] * 8 + place[1] * 2 + target) * COLS
        return pltpu.make_async_remote_copy(
            src_ref=train.at[:, pl.ds(pl.multiple_of(column, 128), COLS)],
            dst_ref=recv.at[pl.ds(pl.multiple_of(me * ROWS, ROWS), ROWS)],
            send_sem=big_send.at[2 * i + target],
            recv_sem=big_recv.at[2 * i + core],
            device_id=(place[0], place[1], target, y),
            device_id_type=MESH,
        )

    def small(ref, send, got, k, there):
        return pltpu.make_async_remote_copy(
            src_ref=ref, dst_ref=ref, send_sem=send.at[k], recv_sem=got.at[k],
            device_id=there, device_id_type=MESH,
        )

    pl.semaphore_wait(barrier, len(NEAR) + 3)
    other = pltpu.make_async_remote_copy(
        src_ref=train.at[:, pl.ds(pl.multiple_of((chip * 2 + 1 - core) * COLS, 128), COLS)],
        dst_ref=recv.at[pl.ds(pl.multiple_of(me * ROWS, ROWS), ROWS)],
        send_sem=big_send.at[30],
        recv_sem=big_recv.at[30],
        device_id=at(0, 0, 1),
        device_id_type=MESH,
    )
    bigs = [
        big(at(dz, dx, 0), i, target) for i, (dz, dx) in enumerate(CHIPS) for target in range(2)
    ]
    other.start()
    for copy in bigs[: 2 * EARLY]:
        copy.start()
    for dz, dx, dc in NEAR:
        pl.semaphore_signal(heard, inc=1, device_id=at(dz, dx, dc), device_id_type=MESH)
    get_low.wait()
    pl.semaphore_wait(heard, len(NEAR))
    stages = (
        (at(core * d, (1 - core) * d, 0), slot) for d in (1, 2, 3)
    ), (
        (at((1 - core) * d, core * d, 0), line) for d in (1, 2, 3)
    ), (
        (at(0, 0, 0, d), pl.ds(0, 16)) for d in (1, 2, 3)
    )
    started = 2 * EARLY
    for n, (stage, until) in enumerate(zip(stages, (started + MORE, len(bigs), len(bigs)))):
        smalls = []
        for k, (there, part) in enumerate(stage):
            smalls.append(small(low_all.at[core, y, part], low_send, low_recv, 3 * n + k, there))
            smalls.append(small(norm_all.at[core, y, part], norm_send, norm_recv, 3 * n + k, there))
        for copy in smalls:
            copy.start()
        for copy in bigs[started:until]:
            copy.start()
        started = until
        for copy in smalls:
            copy.wait()
    there = at(0, 0, 1)
    smalls = [
        small(low_all.at[core], low_send, low_recv, 9, there),
        small(norm_all.at[core], norm_send, norm_recv, 9, there),
    ]
    for copy in smalls:
        copy.start()
    for copy in smalls:
        copy.wait()

    for c in range(2):
        row = jnp.zeros((16, 384), jnp.float32)
        for q in range(4):
            part = norm_all[c, q].reshape(16, 128)
            part = jnp.concatenate([part, jnp.zeros((16, 256), jnp.float32)], axis=1)
            row = row + (pltpu.roll(part, q * PIECE, 1) if q else part)
        for j in range(3):
            lanes = row[:, j * 128 : j * 128 + 128]
            if c == 0:
                norm_rows[pl.ds(j, 16, stride=6), :] = lanes
            else:
                for i in range(4):
                    norm_rows[pl.ds(6 * i + 3 + j, 4, stride=24), :] = lanes[4 * i : 4 * i + 4]
    norm[...] = norm_rows[...].astype(jnp.bfloat16)

    get_high.wait()
    right = (high_mine[...].astype(jnp.float32) * mix_rate).astype(jnp.bfloat16)

    @pl.loop(0, 32)
    def _(source):
        source_core, source_chip = source % 2, source // 2
        crossed = (source_chip % 4) * 4 + source_chip // 4
        place = source_chip * (1 - source_core) + crossed * source_core
        low_cols[...] = jnp.concatenate(
            [low_all[source_core, q, place].astype(jnp.float32) for q in range(4)], axis=0
        ).T.astype(jnp.bfloat16)

        @pl.loop(0, ROWS // TILE)
        def _(i):
            start = pl.multiple_of(i * TILE, TILE)
            whole[pl.ds(pl.multiple_of(source * ROWS + start, TILE), TILE)] = jnp.dot(
                low_cols[pl.ds(start, TILE)], right, preferred_element_type=jnp.float32
            )

    def add(source):
        @pl.loop(0, ROWS // TILE)
        def _(i):
            rows = pl.ds(pl.multiple_of(source * ROWS + i * TILE, TILE), TILE)
            value = recv[rows].astype(jnp.float32) + whole[rows]
            whole[rows] = value
            sums[...] += jnp.sum(jnp.abs(value).reshape(TILE // 8, 8, COLS), axis=0)

    own.wait()
    add(me)
    other.wait()
    add(chip * 2 + 1 - core)
    for i, (dz, dx) in enumerate(CHIPS):
        from_z, from_x, _, _ = at(4 - dz, 4 - dx, 0)
        for source_core in range(2):
            source = (from_z * 4 + from_x) * 2 + source_core
            pltpu.make_async_remote_copy(
                src_ref=train.at[:, pl.ds(0, COLS)],
                dst_ref=recv.at[pl.ds(pl.multiple_of(source * ROWS, ROWS), ROWS)],
                send_sem=big_send.at[2 * i + source_core],
                recv_sem=big_recv.at[2 * i + source_core],
                device_id=(from_z, from_x, source_core, y),
                device_id_type=MESH,
            ).wait_recv()
            add(source)
    scale[...] = jnp.sum(sums[...], axis=0, keepdims=True) / D_MODEL
    for copy in bigs:
        copy.wait_send()


def finish(whole, scale, norm, serving, scale_out, norm_out, staged, scale_line, sems, small_sems):
    scale_line[...] = scale[0]
    inverse = 1.0 / scale[...]
    copies = [
        pltpu.make_async_copy(scale_line, scale_out, small_sems.at[0]),
        pltpu.make_async_copy(norm, norm_out, small_sems.at[1]),
    ]
    for copy in copies:
        copy.start()
    first = 0
    for i, length in enumerate(PARTS):

        @pl.loop(0, length // BODY)
        def _(j):
            inner = pl.ds(pl.multiple_of(first + j * BODY, BODY), BODY)
            staged[inner] = (whole[inner] * inverse).astype(jnp.bfloat16)

        rows = pl.ds(first, length)
        copy = pltpu.make_async_copy(staged.at[rows], serving.at[rows], sems.at[i])
        copy.start()
        copies.append(copy)
        first += length
    for copy in copies:
        copy.wait()


def local(train_up, low_up, high_up, norm_train, norm_step):
    vmem = pl.BlockSpec(memory_space=pltpu.VMEM)
    hbm = pl.BlockSpec(memory_space=pltpu.HBM)
    dma = pltpu.SemaphoreType.DMA
    inputs = (
        train_up, low_up.T, high_up, norm_train.reshape(1, PIECE), norm_step.reshape(1, PIECE)
    )
    whole, scale, norm = pl.pallas_call(
        exchange,
        name="exchange",
        out_shape=(
            pltpu.VMEM((D_MODEL, COLS), jnp.float32),
            jax.ShapeDtypeStruct((1, COLS), jnp.float32),
            jax.ShapeDtypeStruct((PIECE, 128), jnp.bfloat16),
        ),
        in_specs=[hbm] * 5,
        out_specs=(vmem, vmem, vmem),
        scratch_shapes=[
            pltpu.VMEM((D_MODEL, COLS), jnp.bfloat16),
            pltpu.VMEM((RANK, COLS), jnp.bfloat16),
            pltpu.VMEM((2, 1, PIECE), jnp.float32),
            pltpu.VMEM((ROWS, RANK), jnp.bfloat16),
            pltpu.VMEM((2, 4, 16, 8, ROWS), jnp.bfloat16),
            pltpu.VMEM((2, 4, 16, 1, 128), jnp.float32),
            pltpu.VMEM((8, COLS), jnp.float32),
            pltpu.VMEM((PIECE, 128), jnp.float32),
            pltpu.SemaphoreType.REGULAR, dma((31,)), dma((31,)), dma((10,)), dma((10,)), dma((10,)), dma((10,)), dma((5,)),
        ],
        compiler_params=pltpu.CompilerParams(
            collective_id=0, has_side_effects=True, vmem_limit_bytes=16 << 20
        ),
        cost_estimate=pl.CostEstimate(flops=300_000_000, bytes_accessed=40_000_000, transcendentals=0),
    )(*[pltpu.with_memory_space_constraint(array, pltpu.HBM) for array in inputs])
    serving_up, scale_up, serve_norm = pl.pallas_call(
        finish,
        name="finish",
        out_shape=(
            jax.ShapeDtypeStruct((D_MODEL, COLS), jnp.bfloat16),
            jax.ShapeDtypeStruct((COLS,), jnp.float32),
            jax.ShapeDtypeStruct((PIECE, 128), jnp.bfloat16),
        ),
        in_specs=[vmem, vmem, vmem],
        out_specs=(hbm, hbm, hbm),
        scratch_shapes=[
            pltpu.VMEM((D_MODEL, COLS), jnp.bfloat16),
            pltpu.VMEM((COLS,), jnp.float32),
            dma((len(PARTS),)), dma((2,)),
        ],
        compiler_params=pltpu.CompilerParams(vmem_limit_bytes=12 << 20),
        cost_estimate=pl.CostEstimate(flops=10_000_000, bytes_accessed=10_000_000, transcendentals=0),
    )(pltpu.with_memory_space_constraint(whole, pltpu.VMEM), scale, norm)
    return serving_up, scale_up, serve_norm.reshape(D_MODEL)


def solution(mesh):
    split = Mesh(
        mesh.devices.reshape(4, 4, 2, mesh.shape["model"]), ("zero_0", "zero_1", "zero_2", "model")
    )
    placed = (P(ZERO, "model"), P(ZERO, None), P(None, "model"), P(ZERO_MODEL), P(ZERO_MODEL))
    return jax.shard_map(
        local,
        mesh=split,
        in_specs=placed,
        out_specs=(P(None, MODEL_ZERO), P(MODEL_ZERO), P()),
        check_vma=False,
    )
```

```python
import jax
import jax.numpy as jnp
from jax import lax
from jax.experimental import pallas as pl
from jax.experimental.pallas import tpu as pltpu
from jax.sharding import Mesh
from jax.sharding import PartitionSpec as P

D_MODEL = 12288
ROWS = 384
COLS = 384
RANK = 32
PIECE = 96
ZERO = ("zero_0", "zero_1", "zero_2")
ZERO_MODEL = ("zero_0", "zero_1", "zero_2", "model")
MODEL_ZERO = ("model", "zero_0", "zero_1", "zero_2")
MESH = pl.DeviceIdType.MESH

mix_rate = 0.5

PHASES = (
    ((1, 3), (3, 1)),
    ((1, 1), (3, 3)),
    ((3, 2), (1, 0)),
    ((1, 2), (3, 0)),
    ((2, 3), (0, 1)),
    ((2, 1), (0, 3)),
    ((0, 2),),
    ((2, 2), (2, 0)),
)
FIRST = 2
MORE = 4
CHIPS = tuple((z, x) for phase in PHASES for x, z in phase)
EARLY = sum(len(phase) for phase in PHASES[:FIRST])
NEAR = ((0, 0, 1),) + tuple(
    (z, x, c) for z in (0, 1, 3) for x in (0, 1, 3) for c in range(2) if (z, x) != (0, 0)
)
TILE = 128
PARTS = (256, 512, 768) + (1536,) * 7
BODY = 256


def exchange(
    train, low, high, norm_train, norm_step, whole, scale, norm,
    recv, high_mine, norm_mine, low_cols, low_all, norm_all, sums, norm_rows,
    heard, big_send, big_recv, low_send, low_recv, norm_send, norm_recv, local_sem,
):
    z, x, core, y = (lax.axis_index(a) for a in ZERO_MODEL)
    chip = z * 4 + x
    me = chip * 2 + core
    slot = chip * (1 - core) + (x * 4 + z) * core
    line = pl.ds((z * (1 - core) + x * core) * 4, 4)

    def at(dz, dx, dc, dy=0):
        return (lax.rem(z + dz, 4), lax.rem(x + dx, 4), lax.rem(core + dc, 2), lax.rem(y + dy, 4))

    barrier = pltpu.get_barrier_semaphore()
    for dz, dx, dc in NEAR:
        pl.semaphore_signal(barrier, inc=1, device_id=at(dz, dx, dc), device_id_type=MESH)
    for dy in (1, 2, 3):
        pl.semaphore_signal(barrier, inc=1, device_id=at(0, 0, 0, dy), device_id_type=MESH)

    own = pltpu.make_async_copy(
        train.at[:, pl.ds(pl.multiple_of(me * COLS, 128), COLS)],
        recv.at[pl.ds(pl.multiple_of(me * ROWS, ROWS), ROWS)],
        local_sem.at[0],
    )
    own.start()
    get_high = pltpu.make_async_copy(
        high.at[:, pl.ds(pl.multiple_of(me * COLS, 128), COLS)], high_mine, local_sem.at[1]
    )
    get_high.start()

    get_low = pltpu.make_async_copy(
        low.at[pl.ds(pl.multiple_of(y * 8, 8), 8)], low_all.at[core, y, slot], local_sem.at[2]
    )
    get_low.start()
    get_norm = [
        pltpu.make_async_copy(ref, norm_mine.at[i], local_sem.at[3 + i])
        for i, ref in enumerate((norm_train, norm_step))
    ]
    for copy in get_norm:
        copy.start()
    norm_all[core, y, slot] = jnp.zeros((1, 128), jnp.float32)
    sums[...] = jnp.zeros_like(sums)
    for copy in get_norm:
        copy.wait()
    norm_all[core, y, slot, :, pl.ds(0, PIECE)] = norm_mine[0] + norm_mine[1]

    def big(place, i, target):
        column = (place[0] * 8 + place[1] * 2 + target) * COLS
        return pltpu.make_async_remote_copy(
            src_ref=train.at[:, pl.ds(pl.multiple_of(column, 128), COLS)],
            dst_ref=recv.at[pl.ds(pl.multiple_of(me * ROWS, ROWS), ROWS)],
            send_sem=big_send.at[2 * i + target],
            recv_sem=big_recv.at[2 * i + core],
            device_id=(place[0], place[1], target, y),
            device_id_type=MESH,
        )

    def small(ref, send, got, k, there):
        return pltpu.make_async_remote_copy(
            src_ref=ref, dst_ref=ref, send_sem=send.at[k], recv_sem=got.at[k],
            device_id=there, device_id_type=MESH,
        )

    pl.semaphore_wait(barrier, len(NEAR) + 3)
    other = pltpu.make_async_remote_copy(
        src_ref=train.at[:, pl.ds(pl.multiple_of((chip * 2 + 1 - core) * COLS, 128), COLS)],
        dst_ref=recv.at[pl.ds(pl.multiple_of(me * ROWS, ROWS), ROWS)],
        send_sem=big_send.at[30],
        recv_sem=big_recv.at[30],
        device_id=at(0, 0, 1),
        device_id_type=MESH,
    )
    bigs = [
        big(at(dz, dx, 0), i, target)
        for i, (dz, dx) in enumerate(CHIPS[:-2])
        for target in range(2)
    ]
    across = jnp.minimum(z, 1)
    for turn in (across, 1 - across):
        bigs += [big(at(2 * turn, 2, 0), len(CHIPS) - 1 - turn, target) for target in range(2)]
    other.start()
    for copy in bigs[: 2 * EARLY]:
        copy.start()
    for dz, dx, dc in NEAR:
        pl.semaphore_signal(heard, inc=1, device_id=at(dz, dx, dc), device_id_type=MESH)
    get_low.wait()
    pl.semaphore_wait(heard, len(NEAR))
    stages = (
        (at(core * d, (1 - core) * d, 0), slot) for d in (1, 2, 3)
    ), (
        (at((1 - core) * d, core * d, 0), line) for d in (1, 2, 3)
    ), (
        (at(0, 0, 0, d), pl.ds(0, 16)) for d in (1, 2, 3)
    )
    started = 2 * EARLY
    for n, (stage, until) in enumerate(zip(stages, (started + MORE, len(bigs), len(bigs)))):
        smalls = []
        for k, (there, part) in enumerate(stage):
            smalls.append(small(low_all.at[core, y, part], low_send, low_recv, 3 * n + k, there))
            smalls.append(small(norm_all.at[core, y, part], norm_send, norm_recv, 3 * n + k, there))
        for copy in smalls:
            copy.start()
        for copy in bigs[started:until]:
            copy.start()
        started = until
        for copy in smalls:
            copy.wait()
    there = at(0, 0, 1)
    smalls = [
        small(low_all.at[core], low_send, low_recv, 9, there),
        small(norm_all.at[core], norm_send, norm_recv, 9, there),
    ]
    for copy in smalls:
        copy.start()
    for copy in smalls:
        copy.wait()

    for c in range(2):
        row = jnp.zeros((16, 384), jnp.float32)
        for q in range(4):
            part = norm_all[c, q].reshape(16, 128)
            part = jnp.concatenate([part, jnp.zeros((16, 256), jnp.float32)], axis=1)
            row = row + (pltpu.roll(part, q * PIECE, 1) if q else part)
        for j in range(3):
            lanes = row[:, j * 128 : j * 128 + 128]
            if c == 0:
                norm_rows[pl.ds(j, 16, stride=6), :] = lanes
            else:
                for i in range(4):
                    norm_rows[pl.ds(6 * i + 3 + j, 4, stride=24), :] = lanes[4 * i : 4 * i + 4]
    norm[...] = norm_rows[...].astype(jnp.bfloat16)

    get_high.wait()
    right = (high_mine[...].astype(jnp.float32) * mix_rate).astype(jnp.bfloat16)

    @pl.loop(0, 32)
    def _(source):
        source_core, source_chip = source % 2, source // 2
        crossed = (source_chip % 4) * 4 + source_chip // 4
        place = source_chip * (1 - source_core) + crossed * source_core
        low_cols[...] = jnp.concatenate(
            [low_all[source_core, q, place].astype(jnp.float32) for q in range(4)], axis=0
        ).T.astype(jnp.bfloat16)

        @pl.loop(0, ROWS // TILE)
        def _(i):
            start = pl.multiple_of(i * TILE, TILE)
            whole[pl.ds(pl.multiple_of(source * ROWS + start, TILE), TILE)] = jnp.dot(
                low_cols[pl.ds(start, TILE)], right, preferred_element_type=jnp.float32
            )

    def add(source):
        @pl.loop(0, ROWS // TILE)
        def _(i):
            rows = pl.ds(pl.multiple_of(source * ROWS + i * TILE, TILE), TILE)
            value = recv[rows].astype(jnp.float32) + whole[rows]
            whole[rows] = value
            sums[...] += jnp.sum(jnp.abs(value).reshape(TILE // 8, 8, COLS), axis=0)

    own.wait()
    add(me)
    other.wait()
    add(chip * 2 + 1 - core)
    for i, (dz, dx) in enumerate(CHIPS):
        from_z, from_x, _, _ = at(4 - dz, 4 - dx, 0)
        for source_core in range(2):
            source = (from_z * 4 + from_x) * 2 + source_core
            pltpu.make_async_remote_copy(
                src_ref=train.at[:, pl.ds(0, COLS)],
                dst_ref=recv.at[pl.ds(pl.multiple_of(source * ROWS, ROWS), ROWS)],
                send_sem=big_send.at[2 * i + source_core],
                recv_sem=big_recv.at[2 * i + source_core],
                device_id=(from_z, from_x, source_core, y),
                device_id_type=MESH,
            ).wait_recv()
            add(source)
    scale[...] = jnp.sum(sums[...], axis=0, keepdims=True) / D_MODEL
    for copy in bigs:
        copy.wait_send()


def finish(whole, scale, norm, serving, scale_out, norm_out, staged, scale_line, sems, small_sems):
    scale_line[...] = scale[0]
    inverse = 1.0 / scale[...]
    copies = [
        pltpu.make_async_copy(scale_line, scale_out, small_sems.at[0]),
        pltpu.make_async_copy(norm, norm_out, small_sems.at[1]),
    ]
    for copy in copies:
        copy.start()
    first = 0
    for i, length in enumerate(PARTS):

        @pl.loop(0, length // BODY)
        def _(j):
            inner = pl.ds(pl.multiple_of(first + j * BODY, BODY), BODY)
            staged[inner] = (whole[inner] * inverse).astype(jnp.bfloat16)

        rows = pl.ds(first, length)
        copy = pltpu.make_async_copy(staged.at[rows], serving.at[rows], sems.at[i])
        copy.start()
        copies.append(copy)
        first += length
    for copy in copies:
        copy.wait()


def local(train_up, low_up, high_up, norm_train, norm_step):
    vmem = pl.BlockSpec(memory_space=pltpu.VMEM)
    hbm = pl.BlockSpec(memory_space=pltpu.HBM)
    dma = pltpu.SemaphoreType.DMA
    inputs = (
        train_up, low_up.T, high_up, norm_train.reshape(1, PIECE), norm_step.reshape(1, PIECE)
    )
    whole, scale, norm = pl.pallas_call(
        exchange,
        name="exchange",
        out_shape=(
            pltpu.VMEM((D_MODEL, COLS), jnp.float32),
            jax.ShapeDtypeStruct((1, COLS), jnp.float32),
            jax.ShapeDtypeStruct((PIECE, 128), jnp.bfloat16),
        ),
        in_specs=[hbm] * 5,
        out_specs=(vmem, vmem, vmem),
        scratch_shapes=[
            pltpu.VMEM((D_MODEL, COLS), jnp.bfloat16),
            pltpu.VMEM((RANK, COLS), jnp.bfloat16),
            pltpu.VMEM((2, 1, PIECE), jnp.float32),
            pltpu.VMEM((ROWS, RANK), jnp.bfloat16),
            pltpu.VMEM((2, 4, 16, 8, ROWS), jnp.bfloat16),
            pltpu.VMEM((2, 4, 16, 1, 128), jnp.float32),
            pltpu.VMEM((8, COLS), jnp.float32),
            pltpu.VMEM((PIECE, 128), jnp.float32),
            pltpu.SemaphoreType.REGULAR, dma((31,)), dma((31,)), dma((10,)), dma((10,)), dma((10,)), dma((10,)), dma((5,)),
        ],
        compiler_params=pltpu.CompilerParams(
            collective_id=0, has_side_effects=True, vmem_limit_bytes=16 << 20
        ),
        cost_estimate=pl.CostEstimate(flops=300_000_000, bytes_accessed=40_000_000, transcendentals=0),
    )(*[pltpu.with_memory_space_constraint(array, pltpu.HBM) for array in inputs])
    serving_up, scale_up, serve_norm = pl.pallas_call(
        finish,
        name="finish",
        out_shape=(
            jax.ShapeDtypeStruct((D_MODEL, COLS), jnp.bfloat16),
            jax.ShapeDtypeStruct((COLS,), jnp.float32),
            jax.ShapeDtypeStruct((PIECE, 128), jnp.bfloat16),
        ),
        in_specs=[vmem, vmem, vmem],
        out_specs=(hbm, hbm, hbm),
        scratch_shapes=[
            pltpu.VMEM((D_MODEL, COLS), jnp.bfloat16),
            pltpu.VMEM((COLS,), jnp.float32),
            dma((len(PARTS),)), dma((2,)),
        ],
        compiler_params=pltpu.CompilerParams(vmem_limit_bytes=12 << 20),
        cost_estimate=pl.CostEstimate(flops=10_000_000, bytes_accessed=10_000_000, transcendentals=0),
    )(pltpu.with_memory_space_constraint(whole, pltpu.VMEM), scale, norm)
    return serving_up, scale_up, serve_norm.reshape(D_MODEL)


def solution(mesh):
    split = Mesh(
        mesh.devices.reshape(4, 4, 2, mesh.shape["model"]), ("zero_0", "zero_1", "zero_2", "model")
    )
    placed = (P(ZERO, "model"), P(ZERO, None), P(None, "model"), P(ZERO_MODEL), P(ZERO_MODEL))
    return jax.shard_map(
        local,
        mesh=split,
        in_specs=placed,
        out_specs=(P(None, MODEL_ZERO), P(MODEL_ZERO), P()),
        check_vma=False,
    )
```

```python
import jax
import jax.numpy as jnp
from jax import lax
from jax.experimental import pallas as pl
from jax.experimental.pallas import tpu as pltpu
from jax.sharding import Mesh
from jax.sharding import PartitionSpec as P

D_MODEL = 12288
ROWS = 384
COLS = 384
RANK = 32
PIECE = 96
ZERO = ("zero_0", "zero_1", "zero_2")
ZERO_MODEL = ("zero_0", "zero_1", "zero_2", "model")
MODEL_ZERO = ("model", "zero_0", "zero_1", "zero_2")
MESH = pl.DeviceIdType.MESH

mix_rate = 0.5

PHASES = (
    ((1, 3), (3, 1)),
    ((1, 1), (3, 3)),
    ((3, 2), (1, 0)),
    ((1, 2), (3, 0)),
    ((2, 3), (0, 1)),
    ((2, 1), (0, 3)),
    ((2, 2),),
    ((2, 0), (0, 2)),
)
FIRST = 2
MORE = 8
CHIPS = tuple((z, x) for phase in PHASES for x, z in phase)
EARLY = sum(len(phase) for phase in PHASES[:FIRST])
NEAR = ((0, 0, 1),) + tuple(
    (z, x, c) for z in (0, 1, 3) for x in (0, 1, 3) for c in range(2) if (z, x) != (0, 0)
)
TILE = 128
PARTS = (256, 512, 768) + (1536,) * 7
BODY = 256


def exchange(
    train, low, high, norm_train, norm_step, whole, scale, norm,
    recv, high_mine, norm_mine, low_cols, low_all, norm_all, sums, norm_rows,
    heard, big_send, big_recv, low_send, low_recv, norm_send, norm_recv, local_sem,
):
    z, x, core, y = (lax.axis_index(a) for a in ZERO_MODEL)
    chip = z * 4 + x
    me = chip * 2 + core
    slot = chip * (1 - core) + (x * 4 + z) * core
    line = pl.ds((z * (1 - core) + x * core) * 4, 4)

    def at(dz, dx, dc, dy=0):
        return (lax.rem(z + dz, 4), lax.rem(x + dx, 4), lax.rem(core + dc, 2), lax.rem(y + dy, 4))

    barrier = pltpu.get_barrier_semaphore()
    for dz, dx, dc in NEAR:
        pl.semaphore_signal(barrier, inc=1, device_id=at(dz, dx, dc), device_id_type=MESH)
    for dy in (1, 2, 3):
        pl.semaphore_signal(barrier, inc=1, device_id=at(0, 0, 0, dy), device_id_type=MESH)

    own = pltpu.make_async_copy(
        train.at[:, pl.ds(pl.multiple_of(me * COLS, 128), COLS)],
        recv.at[pl.ds(pl.multiple_of(me * ROWS, ROWS), ROWS)],
        local_sem.at[0],
    )
    own.start()
    get_high = pltpu.make_async_copy(
        high.at[:, pl.ds(pl.multiple_of(me * COLS, 128), COLS)], high_mine, local_sem.at[1]
    )
    get_high.start()

    get_low = pltpu.make_async_copy(
        low.at[pl.ds(pl.multiple_of(y * 8, 8), 8)], low_all.at[core, y, slot], local_sem.at[2]
    )
    get_low.start()
    get_norm = [
        pltpu.make_async_copy(ref, norm_mine.at[i], local_sem.at[3 + i])
        for i, ref in enumerate((norm_train, norm_step))
    ]
    for copy in get_norm:
        copy.start()
    norm_all[core, y, slot] = jnp.zeros((1, 128), jnp.float32)
    sums[...] = jnp.zeros_like(sums)
    for copy in get_norm:
        copy.wait()
    norm_all[core, y, slot, :, pl.ds(0, PIECE)] = norm_mine[0] + norm_mine[1]

    def big(place, i, target):
        column = (place[0] * 8 + place[1] * 2 + target) * COLS
        return pltpu.make_async_remote_copy(
            src_ref=train.at[:, pl.ds(pl.multiple_of(column, 128), COLS)],
            dst_ref=recv.at[pl.ds(pl.multiple_of(me * ROWS, ROWS), ROWS)],
            send_sem=big_send.at[2 * i + target],
            recv_sem=big_recv.at[2 * i + core],
            device_id=(place[0], place[1], target, y),
            device_id_type=MESH,
        )

    def small(ref, send, got, k, there):
        return pltpu.make_async_remote_copy(
            src_ref=ref, dst_ref=ref, send_sem=send.at[k], recv_sem=got.at[k],
            device_id=there, device_id_type=MESH,
        )

    pl.semaphore_wait(barrier, len(NEAR) + 3)
    other = pltpu.make_async_remote_copy(
        src_ref=train.at[:, pl.ds(pl.multiple_of((chip * 2 + 1 - core) * COLS, 128), COLS)],
        dst_ref=recv.at[pl.ds(pl.multiple_of(me * ROWS, ROWS), ROWS)],
        send_sem=big_send.at[30],
        recv_sem=big_recv.at[30],
        device_id=at(0, 0, 1),
        device_id_type=MESH,
    )
    bigs = [
        big(at(dz, dx, 0), i, target) for i, (dz, dx) in enumerate(CHIPS) for target in range(2)
    ]
    other.start()
    for copy in bigs[: 2 * EARLY]:
        copy.start()
    for dz, dx, dc in NEAR:
        pl.semaphore_signal(heard, inc=1, device_id=at(dz, dx, dc), device_id_type=MESH)
    get_low.wait()
    pl.semaphore_wait(heard, len(NEAR))
    stages = (
        (at(core * d, (1 - core) * d, 0), slot) for d in (1, 2, 3)
    ), (
        (at((1 - core) * d, core * d, 0), line) for d in (1, 2, 3)
    ), (
        (at(0, 0, 0, d), pl.ds(0, 16)) for d in (1, 2, 3)
    )
    started = 2 * EARLY
    for n, (stage, until) in enumerate(zip(stages, (started + MORE, len(bigs), len(bigs)))):
        smalls = []
        for k, (there, part) in enumerate(stage):
            smalls.append(small(low_all.at[core, y, part], low_send, low_recv, 3 * n + k, there))
            smalls.append(small(norm_all.at[core, y, part], norm_send, norm_recv, 3 * n + k, there))
        for copy in smalls:
            copy.start()
        for copy in bigs[started:until]:
            copy.start()
        started = until
        for copy in smalls:
            copy.wait()
    there = at(0, 0, 1)
    smalls = [
        small(low_all.at[core], low_send, low_recv, 9, there),
        small(norm_all.at[core], norm_send, norm_recv, 9, there),
    ]
    for copy in smalls:
        copy.start()
    for copy in smalls:
        copy.wait()

    for c in range(2):
        row = jnp.zeros((16, 384), jnp.float32)
        for q in range(4):
            part = norm_all[c, q].reshape(16, 128)
            part = jnp.concatenate([part, jnp.zeros((16, 256), jnp.float32)], axis=1)
            row = row + (pltpu.roll(part, q * PIECE, 1) if q else part)
        for j in range(3):
            lanes = row[:, j * 128 : j * 128 + 128]
            if c == 0:
                norm_rows[pl.ds(j, 16, stride=6), :] = lanes
            else:
                for i in range(4):
                    norm_rows[pl.ds(6 * i + 3 + j, 4, stride=24), :] = lanes[4 * i : 4 * i + 4]
    norm[...] = norm_rows[...].astype(jnp.bfloat16)

    get_high.wait()
    right = (high_mine[...].astype(jnp.float32) * mix_rate).astype(jnp.bfloat16)

    @pl.loop(0, 32)
    def _(source):
        source_core, source_chip = source % 2, source // 2
        crossed = (source_chip % 4) * 4 + source_chip // 4
        place = source_chip * (1 - source_core) + crossed * source_core
        low_cols[...] = jnp.concatenate(
            [low_all[source_core, q, place].astype(jnp.float32) for q in range(4)], axis=0
        ).T.astype(jnp.bfloat16)

        @pl.loop(0, ROWS // TILE)
        def _(i):
            start = pl.multiple_of(i * TILE, TILE)
            whole[pl.ds(pl.multiple_of(source * ROWS + start, TILE), TILE)] = jnp.dot(
                low_cols[pl.ds(start, TILE)], right, preferred_element_type=jnp.float32
            )

    def add(source):
        @pl.loop(0, ROWS // TILE)
        def _(i):
            rows = pl.ds(pl.multiple_of(source * ROWS + i * TILE, TILE), TILE)
            value = recv[rows].astype(jnp.float32) + whole[rows]
            whole[rows] = value
            sums[...] += jnp.sum(jnp.abs(value).reshape(TILE // 8, 8, COLS), axis=0)

    own.wait()
    add(me)
    other.wait()
    add(chip * 2 + 1 - core)
    for i, (dz, dx) in enumerate(CHIPS):
        from_z, from_x, _, _ = at(4 - dz, 4 - dx, 0)
        for source_core in range(2):
            source = (from_z * 4 + from_x) * 2 + source_core
            pltpu.make_async_remote_copy(
                src_ref=train.at[:, pl.ds(0, COLS)],
                dst_ref=recv.at[pl.ds(pl.multiple_of(source * ROWS, ROWS), ROWS)],
                send_sem=big_send.at[2 * i + source_core],
                recv_sem=big_recv.at[2 * i + source_core],
                device_id=(from_z, from_x, source_core, y),
                device_id_type=MESH,
            ).wait_recv()
            add(source)
    scale[...] = jnp.sum(sums[...], axis=0, keepdims=True) / D_MODEL
    for copy in bigs:
        copy.wait_send()


def finish(whole, scale, norm, serving, scale_out, norm_out, staged, scale_line, sems, small_sems):
    scale_line[...] = scale[0]
    inverse = 1.0 / scale[...]
    copies = [
        pltpu.make_async_copy(scale_line, scale_out, small_sems.at[0]),
        pltpu.make_async_copy(norm, norm_out, small_sems.at[1]),
    ]
    for copy in copies:
        copy.start()
    first = 0
    for i, length in enumerate(PARTS):

        @pl.loop(0, length // BODY)
        def _(j):
            inner = pl.ds(pl.multiple_of(first + j * BODY, BODY), BODY)
            staged[inner] = (whole[inner] * inverse).astype(jnp.bfloat16)

        rows = pl.ds(first, length)
        copy = pltpu.make_async_copy(staged.at[rows], serving.at[rows], sems.at[i])
        copy.start()
        copies.append(copy)
        first += length
    for copy in copies:
        copy.wait()


def local(train_up, low_up, high_up, norm_train, norm_step):
    vmem = pl.BlockSpec(memory_space=pltpu.VMEM)
    hbm = pl.BlockSpec(memory_space=pltpu.HBM)
    dma = pltpu.SemaphoreType.DMA
    inputs = (
        train_up, low_up.T, high_up, norm_train.reshape(1, PIECE), norm_step.reshape(1, PIECE)
    )
    whole, scale, norm = pl.pallas_call(
        exchange,
        name="exchange",
        out_shape=(
            pltpu.VMEM((D_MODEL, COLS), jnp.float32),
            jax.ShapeDtypeStruct((1, COLS), jnp.float32),
            jax.ShapeDtypeStruct((PIECE, 128), jnp.bfloat16),
        ),
        in_specs=[hbm] * 5,
        out_specs=(vmem, vmem, vmem),
        scratch_shapes=[
            pltpu.VMEM((D_MODEL, COLS), jnp.bfloat16),
            pltpu.VMEM((RANK, COLS), jnp.bfloat16),
            pltpu.VMEM((2, 1, PIECE), jnp.float32),
            pltpu.VMEM((ROWS, RANK), jnp.bfloat16),
            pltpu.VMEM((2, 4, 16, 8, ROWS), jnp.bfloat16),
            pltpu.VMEM((2, 4, 16, 1, 128), jnp.float32),
            pltpu.VMEM((8, COLS), jnp.float32),
            pltpu.VMEM((PIECE, 128), jnp.float32),
            pltpu.SemaphoreType.REGULAR, dma((31,)), dma((31,)), dma((10,)), dma((10,)), dma((10,)), dma((10,)), dma((5,)),
        ],
        compiler_params=pltpu.CompilerParams(
            collective_id=0, has_side_effects=True, vmem_limit_bytes=16 << 20
        ),
        cost_estimate=pl.CostEstimate(flops=300_000_000, bytes_accessed=40_000_000, transcendentals=0),
    )(*[pltpu.with_memory_space_constraint(array, pltpu.HBM) for array in inputs])
    serving_up, scale_up, serve_norm = pl.pallas_call(
        finish,
        name="finish",
        out_shape=(
            jax.ShapeDtypeStruct((D_MODEL, COLS), jnp.bfloat16),
            jax.ShapeDtypeStruct((COLS,), jnp.float32),
            jax.ShapeDtypeStruct((PIECE, 128), jnp.bfloat16),
        ),
        in_specs=[vmem, vmem, vmem],
        out_specs=(hbm, hbm, hbm),
        scratch_shapes=[
            pltpu.VMEM((D_MODEL, COLS), jnp.bfloat16),
            pltpu.VMEM((COLS,), jnp.float32),
            dma((len(PARTS),)), dma((2,)),
        ],
        compiler_params=pltpu.CompilerParams(vmem_limit_bytes=12 << 20),
        cost_estimate=pl.CostEstimate(flops=10_000_000, bytes_accessed=10_000_000, transcendentals=0),
    )(pltpu.with_memory_space_constraint(whole, pltpu.VMEM), scale, norm)
    return serving_up, scale_up, serve_norm.reshape(D_MODEL)


def solution(mesh):
    split = Mesh(
        mesh.devices.reshape(4, 4, 2, mesh.shape["model"]), ("zero_0", "zero_1", "zero_2", "model")
    )
    placed = (P(ZERO, "model"), P(ZERO, None), P(None, "model"), P(ZERO_MODEL), P(ZERO_MODEL))
    return jax.shard_map(
        local,
        mesh=split,
        in_specs=placed,
        out_specs=(P(None, MODEL_ZERO), P(MODEL_ZERO), P()),
        check_vma=False,
    )
```

```python
import jax
import jax.numpy as jnp
from jax import lax
from jax.experimental import pallas as pl
from jax.experimental.pallas import tpu as pltpu
from jax.sharding import Mesh
from jax.sharding import PartitionSpec as P

D_MODEL = 12288
ROWS = 384
COLS = 384
RANK = 32
PIECE = 96
ZERO = ("zero_0", "zero_1", "zero_2")
ZERO_MODEL = ("zero_0", "zero_1", "zero_2", "model")
MODEL_ZERO = ("model", "zero_0", "zero_1", "zero_2")
MESH = pl.DeviceIdType.MESH

mix_rate = 0.5

PHASES = (
    ((1, 3), (3, 1)),
    ((1, 1), (3, 3)),
    ((3, 2), (1, 0)),
    ((1, 2), (3, 0)),
    ((2, 3), (0, 1)),
    ((2, 1), (0, 3)),
    ((2, 2),),
    ((2, 0), (0, 2)),
)
FIRST = 2
MORE = 8
CHIPS = tuple((z, x) for phase in PHASES for x, z in phase)
EARLY = sum(len(phase) for phase in PHASES[:FIRST])
NEAR = ((0, 0, 1),) + tuple(
    (z, x, c) for z in (0, 1, 3) for x in (0, 1, 3) for c in range(2) if (z, x) != (0, 0)
)
TILE = 128
PARTS = (256, 512, 768) + (1536,) * 7
BODY = 256


def exchange(
    train, low, high, norm_train, norm_step, whole, scale, norm,
    recv, high_mine, norm_mine, low_cols, low_all, norm_all, sums, norm_rows,
    heard, big_send, big_recv, low_send, low_recv, norm_send, norm_recv, local_sem,
):
    z, x, core, y = (lax.axis_index(a) for a in ZERO_MODEL)
    chip = z * 4 + x
    me = chip * 2 + core
    slot = chip * (1 - core) + (x * 4 + z) * core
    line = pl.ds((z * (1 - core) + x * core) * 4, 4)

    def at(dz, dx, dc, dy=0):
        return (lax.rem(z + dz, 4), lax.rem(x + dx, 4), lax.rem(core + dc, 2), lax.rem(y + dy, 4))

    barrier = pltpu.get_barrier_semaphore()
    for dz, dx, dc in NEAR:
        pl.semaphore_signal(barrier, inc=1, device_id=at(dz, dx, dc), device_id_type=MESH)
    for dy in (1, 2, 3):
        pl.semaphore_signal(barrier, inc=1, device_id=at(0, 0, 0, dy), device_id_type=MESH)

    own = pltpu.make_async_copy(
        train.at[:, pl.ds(pl.multiple_of(me * COLS, 128), COLS)],
        recv.at[pl.ds(pl.multiple_of(me * ROWS, ROWS), ROWS)],
        local_sem.at[0],
    )
    own.start()
    get_high = pltpu.make_async_copy(
        high.at[:, pl.ds(pl.multiple_of(me * COLS, 128), COLS)], high_mine, local_sem.at[1]
    )
    get_high.start()

    get_low = pltpu.make_async_copy(
        low.at[pl.ds(pl.multiple_of(y * 8, 8), 8)], low_all.at[core, y, slot], local_sem.at[2]
    )
    get_low.start()
    get_norm = [
        pltpu.make_async_copy(ref, norm_mine.at[i], local_sem.at[3 + i])
        for i, ref in enumerate((norm_train, norm_step))
    ]
    for copy in get_norm:
        copy.start()

    def big(place, i, target):
        column = (place[0] * 8 + place[1] * 2 + target) * COLS
        return pltpu.make_async_remote_copy(
            src_ref=train.at[:, pl.ds(pl.multiple_of(column, 128), COLS)],
            dst_ref=recv.at[pl.ds(pl.multiple_of(me * ROWS, ROWS), ROWS)],
            send_sem=big_send.at[2 * i + target],
            recv_sem=big_recv.at[2 * i + core],
            device_id=(place[0], place[1], target, y),
            device_id_type=MESH,
        )

    def small(ref, send, got, k, there):
        return pltpu.make_async_remote_copy(
            src_ref=ref, dst_ref=ref, send_sem=send.at[k], recv_sem=got.at[k],
            device_id=there, device_id_type=MESH,
        )

    pl.semaphore_wait(barrier, len(NEAR) + 3)
    other = pltpu.make_async_remote_copy(
        src_ref=train.at[:, pl.ds(pl.multiple_of((chip * 2 + 1 - core) * COLS, 128), COLS)],
        dst_ref=recv.at[pl.ds(pl.multiple_of(me * ROWS, ROWS), ROWS)],
        send_sem=big_send.at[30],
        recv_sem=big_recv.at[30],
        device_id=at(0, 0, 1),
        device_id_type=MESH,
    )
    bigs = [
        big(at(dz, dx, 0), i, target) for i, (dz, dx) in enumerate(CHIPS) for target in range(2)
    ]
    other.start()
    for copy in bigs[: 2 * EARLY]:
        copy.start()
    for dz, dx, dc in NEAR:
        pl.semaphore_signal(heard, inc=1, device_id=at(dz, dx, dc), device_id_type=MESH)
    norm_all[core, y, slot] = jnp.zeros((1, 128), jnp.float32)
    sums[...] = jnp.zeros_like(sums)
    for copy in get_norm:
        copy.wait()
    norm_all[core, y, slot, :, pl.ds(0, PIECE)] = norm_mine[0] + norm_mine[1]
    get_low.wait()
    pl.semaphore_wait(heard, len(NEAR))
    stages = (
        (at(core * d, (1 - core) * d, 0), slot) for d in (1, 2, 3)
    ), (
        (at((1 - core) * d, core * d, 0), line) for d in (1, 2, 3)
    ), (
        (at(0, 0, 0, d), pl.ds(0, 16)) for d in (1, 2, 3)
    )
    started = 2 * EARLY
    for n, (stage, until) in enumerate(zip(stages, (started + MORE, len(bigs), len(bigs)))):
        smalls = []
        for k, (there, part) in enumerate(stage):
            smalls.append(small(low_all.at[core, y, part], low_send, low_recv, 3 * n + k, there))
            smalls.append(small(norm_all.at[core, y, part], norm_send, norm_recv, 3 * n + k, there))
        for copy in smalls:
            copy.start()
        for copy in bigs[started:until]:
            copy.start()
        started = until
        for copy in smalls:
            copy.wait()
    there = at(0, 0, 1)
    smalls = [
        small(low_all.at[core], low_send, low_recv, 9, there),
        small(norm_all.at[core], norm_send, norm_recv, 9, there),
    ]
    for copy in smalls:
        copy.start()
    for copy in smalls:
        copy.wait()

    for c in range(2):
        row = jnp.zeros((16, 384), jnp.float32)
        for q in range(4):
            part = norm_all[c, q].reshape(16, 128)
            part = jnp.concatenate([part, jnp.zeros((16, 256), jnp.float32)], axis=1)
            row = row + (pltpu.roll(part, q * PIECE, 1) if q else part)
        for j in range(3):
            lanes = row[:, j * 128 : j * 128 + 128]
            if c == 0:
                norm_rows[pl.ds(j, 16, stride=6), :] = lanes
            else:
                for i in range(4):
                    norm_rows[pl.ds(6 * i + 3 + j, 4, stride=24), :] = lanes[4 * i : 4 * i + 4]
    norm[...] = norm_rows[...].astype(jnp.bfloat16)

    get_high.wait()
    right = (high_mine[...].astype(jnp.float32) * mix_rate).astype(jnp.bfloat16)

    @pl.loop(0, 32)
    def _(source):
        source_core, source_chip = source % 2, source // 2
        crossed = (source_chip % 4) * 4 + source_chip // 4
        place = source_chip * (1 - source_core) + crossed * source_core
        low_cols[...] = jnp.concatenate(
            [low_all[source_core, q, place].astype(jnp.float32) for q in range(4)], axis=0
        ).T.astype(jnp.bfloat16)

        @pl.loop(0, ROWS // TILE)
        def _(i):
            start = pl.multiple_of(i * TILE, TILE)
            whole[pl.ds(pl.multiple_of(source * ROWS + start, TILE), TILE)] = jnp.dot(
                low_cols[pl.ds(start, TILE)], right, preferred_element_type=jnp.float32
            )

    def add(source):
        @pl.loop(0, ROWS // TILE)
        def _(i):
            rows = pl.ds(pl.multiple_of(source * ROWS + i * TILE, TILE), TILE)
            value = recv[rows].astype(jnp.float32) + whole[rows]
            whole[rows] = value
            sums[...] += jnp.sum(jnp.abs(value).reshape(TILE // 8, 8, COLS), axis=0)

    own.wait()
    add(me)
    other.wait()
    add(chip * 2 + 1 - core)
    for i, (dz, dx) in enumerate(CHIPS):
        from_z, from_x, _, _ = at(4 - dz, 4 - dx, 0)
        for source_core in range(2):
            source = (from_z * 4 + from_x) * 2 + source_core
            pltpu.make_async_remote_copy(
                src_ref=train.at[:, pl.ds(0, COLS)],
                dst_ref=recv.at[pl.ds(pl.multiple_of(source * ROWS, ROWS), ROWS)],
                send_sem=big_send.at[2 * i + source_core],
                recv_sem=big_recv.at[2 * i + source_core],
                device_id=(from_z, from_x, source_core, y),
                device_id_type=MESH,
            ).wait_recv()
            add(source)
    scale[...] = jnp.sum(sums[...], axis=0, keepdims=True) / D_MODEL
    for copy in bigs:
        copy.wait_send()


def finish(whole, scale, norm, serving, scale_out, norm_out, staged, scale_line, sems, small_sems):
    scale_line[...] = scale[0]
    inverse = 1.0 / scale[...]
    copies = [
        pltpu.make_async_copy(scale_line, scale_out, small_sems.at[0]),
        pltpu.make_async_copy(norm, norm_out, small_sems.at[1]),
    ]
    for copy in copies:
        copy.start()
    first = 0
    for i, length in enumerate(PARTS):

        @pl.loop(0, length // BODY)
        def _(j):
            inner = pl.ds(pl.multiple_of(first + j * BODY, BODY), BODY)
            staged[inner] = (whole[inner] * inverse).astype(jnp.bfloat16)

        rows = pl.ds(first, length)
        copy = pltpu.make_async_copy(staged.at[rows], serving.at[rows], sems.at[i])
        copy.start()
        copies.append(copy)
        first += length
    for copy in copies:
        copy.wait()


def local(train_up, low_up, high_up, norm_train, norm_step):
    vmem = pl.BlockSpec(memory_space=pltpu.VMEM)
    hbm = pl.BlockSpec(memory_space=pltpu.HBM)
    dma = pltpu.SemaphoreType.DMA
    inputs = (
        train_up, low_up.T, high_up, norm_train.reshape(1, PIECE), norm_step.reshape(1, PIECE)
    )
    whole, scale, norm = pl.pallas_call(
        exchange,
        name="exchange",
        out_shape=(
            pltpu.VMEM((D_MODEL, COLS), jnp.float32),
            jax.ShapeDtypeStruct((1, COLS), jnp.float32),
            jax.ShapeDtypeStruct((PIECE, 128), jnp.bfloat16),
        ),
        in_specs=[hbm] * 5,
        out_specs=(vmem, vmem, vmem),
        scratch_shapes=[
            pltpu.VMEM((D_MODEL, COLS), jnp.bfloat16),
            pltpu.VMEM((RANK, COLS), jnp.bfloat16),
            pltpu.VMEM((2, 1, PIECE), jnp.float32),
            pltpu.VMEM((ROWS, RANK), jnp.bfloat16),
            pltpu.VMEM((2, 4, 16, 8, ROWS), jnp.bfloat16),
            pltpu.VMEM((2, 4, 16, 1, 128), jnp.float32),
            pltpu.VMEM((8, COLS), jnp.float32),
            pltpu.VMEM((PIECE, 128), jnp.float32),
            pltpu.SemaphoreType.REGULAR, dma((31,)), dma((31,)), dma((10,)), dma((10,)), dma((10,)), dma((10,)), dma((5,)),
        ],
        compiler_params=pltpu.CompilerParams(
            collective_id=0, has_side_effects=True, vmem_limit_bytes=16 << 20
        ),
        cost_estimate=pl.CostEstimate(flops=300_000_000, bytes_accessed=40_000_000, transcendentals=0),
    )(*[pltpu.with_memory_space_constraint(array, pltpu.HBM) for array in inputs])
    serving_up, scale_up, serve_norm = pl.pallas_call(
        finish,
        name="finish",
        out_shape=(
            jax.ShapeDtypeStruct((D_MODEL, COLS), jnp.bfloat16),
            jax.ShapeDtypeStruct((COLS,), jnp.float32),
            jax.ShapeDtypeStruct((PIECE, 128), jnp.bfloat16),
        ),
        in_specs=[vmem, vmem, vmem],
        out_specs=(hbm, hbm, hbm),
        scratch_shapes=[
            pltpu.VMEM((D_MODEL, COLS), jnp.bfloat16),
            pltpu.VMEM((COLS,), jnp.float32),
            dma((len(PARTS),)), dma((2,)),
        ],
        compiler_params=pltpu.CompilerParams(vmem_limit_bytes=12 << 20),
        cost_estimate=pl.CostEstimate(flops=10_000_000, bytes_accessed=10_000_000, transcendentals=0),
    )(pltpu.with_memory_space_constraint(whole, pltpu.VMEM), scale, norm)
    return serving_up, scale_up, serve_norm.reshape(D_MODEL)


def solution(mesh):
    split = Mesh(
        mesh.devices.reshape(4, 4, 2, mesh.shape["model"]), ("zero_0", "zero_1", "zero_2", "model")
    )
    placed = (P(ZERO, "model"), P(ZERO, None), P(None, "model"), P(ZERO_MODEL), P(ZERO_MODEL))
    return jax.shard_map(
        local,
        mesh=split,
        in_specs=placed,
        out_specs=(P(None, MODEL_ZERO), P(MODEL_ZERO), P()),
        check_vma=False,
    )
```
